32 devices in a mesh: dp: 2 (over z, core), tp: 16 (over x, y).
Axes of the slice: x: 4, y: 4, z: 1, core: 2. Of those that a mesh axis runs over, the one named last changes fastest.
The devices are a block of a 4x4x8 slice.
Arguments:
- x: bfloat16 [8192, 4096], P(('dp', 'tp')), parts along dimension 0
- dy: bfloat16 [8192, 4096], P(('dp', 'tp')), parts along dimension 0
- gain: bfloat16 [4096], replicated
- wq: bfloat16 [4096, 4096], P(None, 'tp')
- wk: bfloat16 [4096, 4096], P(None, 'tp')
- wv: bfloat16 [4096, 4096], P(None, 'tp')
- wo: bfloat16 [4096, 4096], P('tp')
Outputs:
- output 1: bfloat16 [8192, 4096], P(('dp', 'tp')), parts along dimension 0
- output 2: float32 [2, 4096], P('dp'), parts along dimension 0
- output 3: bfloat16 [8192, 4096], P('dp', 'tp'), parts along dimension 0
- output 4: bfloat16 [8192, 4096], P('dp', 'tp'), parts along dimension 0
- output 5: bfloat16 [8192, 4096], P('dp', 'tp'), parts along dimension 0
- output 6: bfloat16 [8192, 4096], P(('dp', 'tp')), parts along dimension 0
There are 2 independent parts. The reference program is written for one: setup_inputs(seed, part) draws one part's arguments, and reference() takes and returns one part's arrays. A program takes and returns all parts, laid end to end along the dimension named above; an argument that names none is the same for every part.
All inputs are finite; a program needn't handle non-finite values.
Results may differ from the reference program's by a relative error of at most 0.0187.
Values are sent between devices in bfloat16 or wider.
A program may use at most 768 MiB of HBM per device.

```python
import jax
import jax.numpy as jnp
from jax import lax

ROWS = 4096
D = 4096
HEADS = 16
KV_HEADS = 16
HEAD = 256
THETA = 10000


def setup_inputs(seed: int = 0, part: int = 0) -> dict:
    kx, ky, kn, kq, kk, kv, ko = jax.random.split(jax.random.key(seed), 7)

    def weights(key, rows, columns):
        return jax.random.normal(key, (rows, columns), jnp.float32) * rows**-0.5

    drawn = {
        "x": jax.random.normal(jax.random.fold_in(kx, part), (ROWS, D), jnp.float32),
        "dy": jax.random.normal(jax.random.fold_in(ky, part), (ROWS, D), jnp.float32) * ROWS**-0.5,
        "gain": 1 + 0.1 * jax.random.normal(kn, (D,), jnp.float32),
        "wq": 2 * weights(kq, D, HEADS * HEAD),
        "wk": 2 * weights(kk, D, KV_HEADS * HEAD),
        "wv": 4 * weights(kv, D, KV_HEADS * HEAD),
        "wo": weights(ko, HEADS * HEAD, D),
    }
    return {k: v.astype(jnp.bfloat16) for k, v in drawn.items()}


def normed(x, gain):
    wide = x.astype(jnp.float32)
    scale = lax.rsqrt(jnp.mean(wide * wide, -1, keepdims=True) + 1e-6)
    return (wide * scale * gain.astype(jnp.float32)).astype(jnp.bfloat16)


def turned(t, place, theta):
    half = t.shape[-1] // 2
    angle = place.astype(jnp.float32)[:, None] * theta ** (-jnp.arange(half, dtype=jnp.float32) / half)
    cos, sin = jnp.cos(angle)[:, None], jnp.sin(angle)[:, None]
    a, b = t[..., :half].astype(jnp.float32), t[..., half:].astype(jnp.float32)
    return jnp.concatenate([a * cos - b * sin, b * cos + a * sin], -1).astype(jnp.bfloat16)


def matmul(a, w):
    return jnp.dot(a, w, preferred_element_type=jnp.float32).astype(jnp.bfloat16)


def einsum(form, a, b):
    return jnp.einsum(form, a.astype(jnp.float32), b.astype(jnp.float32))


def attention(q, k, v):
    scores = einsum("tgsd,ugd->gstu", q, k) * q.shape[-1] ** -0.5
    token = jnp.arange(q.shape[0])
    scores = jnp.where(token[:, None] >= token, scores, -jnp.inf)
    weights = jax.nn.softmax(scores, -1).astype(jnp.bfloat16)
    return einsum("gstu,ugd->tgsd", weights, v).astype(jnp.bfloat16)


def forward(x, gain, wq, wk, wv, wo):
    rows = x.shape[0]
    a, place = normed(x, gain), jnp.arange(rows)
    k = turned(matmul(a, wk).reshape(rows, -1, HEAD), place, THETA)
    q = turned(matmul(a, wq).reshape(rows, -1, HEAD), place, THETA).reshape(rows, k.shape[1], -1, HEAD)
    v = matmul(a, wv).reshape(rows, -1, HEAD)
    seen = attention(q, k, v).reshape(rows, -1)
    return (x.astype(jnp.float32) + jnp.dot(seen, wo, preferred_element_type=jnp.float32)).astype(jnp.bfloat16)


def reference(x, dy, gain, wq, wk, wv, wo):
    _, back = jax.vjp(forward, x, gain.astype(jnp.float32), wq, wk, wv, wo)
    by_x, by_gain, *by_weights = back(dy)
    return (by_x, by_gain[None], *by_weights)
```

```python
import functools

import jax
import jax.numpy as jnp
from jax import lax
from jax.experimental import pallas as pl
from jax.experimental.pallas import tpu as pltpu
from jax.sharding import PartitionSpec as P

NEG = -1e30
HIDDEN = 2 * NEG
LOG2E = 1.4426950408889634
VMEM = 62 * 2**20
STRIP = 512
BLOCK = 1024


HEAD = 256
THETA = 10000
SPLIT = 2


def rotations(blocks, rows, half):
    speed = THETA ** (-jnp.arange(half, dtype=jnp.float32) / half)
    first, inside = (jnp.arange(blocks) * rows).astype(jnp.float32)[:, None, None] * speed, jnp.arange(rows).astype(jnp.float32)[:, None] * speed
    return jnp.cos(first), jnp.sin(first), jnp.cos(inside), jnp.sin(inside)


def _angles(turns, block, rows=slice(None)):
    first_cos, first_sin, cos, sin = turns
    c, s, ci, si = first_cos[block], first_sin[block], cos[rows, :], sin[rows, :]
    return c * ci - s * si, s * ci + c * si


def _dot(a, b, ca, cb):
    return lax.dot_general(a, b, (((ca,), (cb,)), ((), ())), preferred_element_type=jnp.float32)


def _visible():
    shape = (STRIP, STRIP)
    return lax.broadcasted_iota(jnp.int32, shape, 1) >= lax.broadcasted_iota(jnp.int32, shape, 0)


def _rows(ref, first, count):
    return ref.at[pl.ds(pl.multiple_of(first, STRIP), count), :]


def _over_keys(iq, block):
    lax.fori_loop(0, iq, lambda j, _: block(j * BLOCK, BLOCK, range(BLOCK // STRIP), None), None)
    for strip in range(BLOCK // STRIP):
        block(iq * BLOCK + strip * STRIP, STRIP, range(strip, BLOCK // STRIP), strip)


def _look(q_ref, k_ref, v_ref, out_ref, lse_ref, top_s, mix_s):
    tokens, head = q_ref.shape
    scale = head**-0.5
    e = scale * LOG2E

    def queries(iq, _):
        top_s[...] = jnp.full(top_s.shape, NEG, jnp.float32)
        mix_s[...] = jnp.zeros(mix_s.shape, jnp.float32)

        def block(first, keys, strips, masked):
            k = _rows(k_ref, first, keys)[...]
            scores = [_dot(k, _rows(q_ref, iq * BLOCK + n * STRIP, STRIP)[...], 1, 1) for n in strips]
            values = jnp.concatenate([_rows(v_ref, first, keys)[...].T, jnp.ones((8, keys), k.dtype)], axis=0)
            weights, keeps = [], []
            for n, s in zip(strips, scores):
                at = slice(n * STRIP, (n + 1) * STRIP)
                if n == masked:
                    s = jnp.where(_visible(), s, HIDDEN)
                old = top_s[:, at]
                top = jnp.maximum(old, s.max(axis=0, keepdims=True))
                top_s[:, at] = top
                weights.append(jnp.exp2((s - top) * e).astype(k.dtype))
                keeps.append(jnp.exp2((old - top) * e))
            for n, p, keep in zip(strips, weights, keeps):
                at = slice(n * STRIP, (n + 1) * STRIP)
                mix_s[:, at] = mix_s[:, at] * keep + _dot(values, p, 1, 0)

        _over_keys(iq, block)
        total = mix_s[head : head + 1, :]
        _rows(out_ref, iq * BLOCK, BLOCK)[...] = (mix_s[:head, :] * (1 / total)).T.astype(out_ref.dtype)
        lse_ref[:, pl.ds(pl.multiple_of(iq * BLOCK, BLOCK), BLOCK)] = top_s[...] * scale + jnp.log(total)

    lax.fori_loop(0, tokens // BLOCK, queries, None)


def _look_back(rel_ref, q_ref, k_ref, v_ref, do_ref, seen_ref, lse_ref, *refs):
    turns, (out_ref, dq_s, dk_s, dv_s) = refs[:4], refs[4:]
    head, low = q_ref.shape[1], q_ref.dtype
    rows, half = out_ref.shape[1], head // 2
    scale = head**-0.5
    e = scale * LOG2E
    iq = pl.program_id(0)

    def finish(block, at, value):
        cos, sin = _angles(turns, block)
        a, b = value[:, :half], value[:, half:]
        place = rel_ref[block]
        out_ref[place, :, at : at + half] = (a * cos + b * sin).astype(low)
        out_ref[place, :, at + half : at + head] = (b * cos - a * sin).astype(low)

    @pl.when(iq == 0)
    def _():
        dk_s[...] = jnp.zeros_like(dk_s)
        dv_s[...] = jnp.zeros_like(dv_s)

    dq_s[...] = jnp.zeros_like(dq_s)
    lse = lse_ref[...] * LOG2E
    delta = (do_ref[...].astype(jnp.float32) * seen_ref[...].astype(jnp.float32)).T.sum(axis=0, keepdims=True)

    def block(first, keys, strips, masked):
        k, v = _rows(k_ref, first, keys)[...], _rows(v_ref, first, keys)[...]
        ats = [slice(n * STRIP, (n + 1) * STRIP) for n in strips]
        qs, dos = [q_ref[at, :] for at in ats], [do_ref[at, :] for at in ats]
        scores = [_dot(k, x, 1, 1) for x in qs]
        dps = [_dot(v, x, 1, 1) for x in dos]
        for n, at, q, do, s, dp in zip(strips, ats, qs, dos, scores, dps):
            p = jnp.exp2(s * e - lse[:, at])
            if n == masked:
                p = jnp.where(_visible(), p, 0.0)
            ds = (p * (dp - delta[:, at])).astype(low)
            dv_at, dk_at = _rows(dv_s, first, keys), _rows(dk_s, first, keys)
            dv_at[...] += _dot(p.astype(low), do, 1, 0)
            dk_at[...] += _dot(ds, q, 1, 0)
            dq_s[:, at] += _dot(k.T, ds, 1, 0)

    _over_keys(iq, block)
    dq = (dq_s[...] * scale).T.astype(low).astype(jnp.float32)
    each = BLOCK // rows
    for i in range(each):
        finish(iq * each + i, 0, dq[i * rows : (i + 1) * rows, :])

    @pl.when(iq == pl.num_programs(0) - 1)
    def _():
        def keys(i, _):
            at = pl.ds(pl.multiple_of(i * rows, rows), rows)
            finish(i, head, (dk_s[at, :] * scale).astype(low).astype(jnp.float32))
            out_ref[rel_ref[i], :, 2 * head :] = dv_s[at, :].astype(low)

        lax.fori_loop(0, out_ref.shape[0], keys, None)


def look_back(rel, q, k, v, do, seen, lse, turns, rows):
    tokens, head = q.shape
    once = dict(pipeline_mode=pl.Buffered(1))
    whole = lambda shape: pl.BlockSpec(shape, lambda i, _: (0,) * len(shape), **once)
    block = pl.BlockSpec((BLOCK, head), lambda i, _: (i, 0))
    out = (tokens // rows, rows, 3 * head)
    return pl.pallas_call(
        _look_back,
        grid_spec=pltpu.PrefetchScalarGridSpec(
            num_scalar_prefetch=1,
            grid=(tokens // BLOCK,),
            in_specs=[block, whole(k.shape), whole(v.shape), block, block, pl.BlockSpec((1, BLOCK), lambda i, _: (0, i)), *[whole(t.shape) for t in turns]],
            out_specs=whole(out),
            scratch_shapes=[pltpu.VMEM((head, BLOCK), jnp.float32), pltpu.VMEM((tokens, head), jnp.float32), pltpu.VMEM((tokens, head), jnp.float32)],
        ),
        out_shape=jax.ShapeDtypeStruct(out, q.dtype),
        compiler_params=pltpu.CompilerParams(dimension_semantics=("arbitrary",), vmem_limit_bytes=VMEM),
        cost_estimate=pl.CostEstimate(flops=5 * tokens * tokens * head, transcendentals=tokens * tokens, bytes_accessed=16 * q.size),
    )(rel, q, k, v, do, seen, lse, *turns)


MESH = pl.DeviceIdType.MESH


def turn_bits(m, s, n):
    return (m * (1 << s)) % n + (m * (1 << s)) // n


def _place(me, flip, bits):
    low = bits // 2
    side = 1 << low
    found = 0
    for at, first in ((me // side, 0), (me % side, low)):
        above, out = 0, 0
        for b in reversed(range(low)):
            bit = (at // (1 << b) + (at // (1 << (b + 1)) if b + 1 < low else 0)) % 2
            bit = (bit + flip // (1 << (first + b))) % 2
            above = (above + bit) % 2
            out = out + above * (1 << b)
        found = found * side + out
    return found


def _gather(bits, x_ref, dy_ref, wq_ref, wk_ref, wv_ref, wo_in, *refs):
    turns, refs = refs[:4], refs[4:]
    all_ref, halves, moved = refs[0], refs[1 : 1 + bits], refs[1 + bits : 1 + 3 * bits]
    q_ref, k_ref, v_ref, seen_ref, lse_ref, d_ref = refs[1 + 3 * bits : 7 + 3 * bits]
    x_s, dy_s, w_s, wo_ref, wo_s, theirs_s, got_s, mine_ref, q_s, k_s, v_s, seen_s, top_s, mix_s = refs[7 + 3 * bits : 21 + 3 * bits]
    x_send, x_recv, dy_send, dy_recv, wo_send, wo_recv, their_send, their_recv, out_sem, local = refs[21 + 3 * bits :]
    n, rows, width = all_ref.shape
    head = q_ref.shape[1]
    half = head // 2
    piece, part = rows // bits, width // bits
    me = lax.axis_index("tp")
    peers = [{"tp": _place(me, 1 << d, bits)} for d in range(bits)]

    barrier = pltpu.get_barrier_semaphore()
    for peer in peers:
        pl.semaphore_signal(barrier, inc=1, device_id=peer, device_id_type=MESH)
    pl.semaphore_wait(barrier, bits)

    def x_piece(m, s):
        return all_ref.at[turn_bits(m, s, n), pl.ds(s * piece, piece), :]

    def x_copy(src, m, k, s):
        return pltpu.make_async_remote_copy(src_ref=src, dst_ref=x_piece(m + (1 << k), s), send_sem=x_send.at[m + (1 << k), s],
                                            recv_sem=x_recv.at[m + (1 << k), s], device_id=peers[(s + k) % bits], device_id_type=MESH)

    def dy_copy(src, m, k, s):
        return pltpu.make_async_remote_copy(src_ref=src, dst_ref=halves[s].at[m + (1 << k)], send_sem=dy_send.at[m + (1 << k), s],
                                            recv_sem=dy_recv.at[m + (1 << k), s], device_id=peers[(s + k) % bits], device_id_type=MESH)

    def wo_copy(s):
        here = (slice(None), pl.ds(s * part, part))
        return pltpu.make_async_remote_copy(src_ref=wo_in.at[here], dst_ref=wo_s.at[here], send_sem=wo_send.at[s], recv_sem=wo_recv.at[s],
                                            device_id=peers[(s + bits - 1) % bits], device_id_type=MESH)

    def their_copy(m, s):
        return pltpu.make_async_remote_copy(src_ref=theirs_s.at[s, m], dst_ref=got_s.at[s, m], send_sem=their_send.at[m, s],
                                            recv_sem=their_recv.at[m, s], device_id=peers[(s + bits - 1) % bits], device_id_type=MESH)

    def seen_copy(m, s, h):
        block = _place(me, turn_bits(m, s, n), bits)
        return pltpu.make_async_copy(seen_s.at[pl.ds(pl.multiple_of(block * rows, rows), rows), :], moved[h * bits + s].at[m % (n // 2)], out_sem.at[m, s])

    for k in range(bits):
        for s in range(bits):
            x_copy(x_ref.at[pl.ds(s * piece, piece), :], 0, k, s).start()
    loads = [pltpu.make_async_copy(a, b, local.at[3 + i]) for i, (a, b) in enumerate([(wq_ref, w_s.at[0]), (wk_ref, w_s.at[1]), (wv_ref, w_s.at[2]), (wo_in, wo_ref)])]
    for load in loads:
        load.start()
    mine_ref[...] = jnp.zeros_like(mine_ref)
    for load in loads:
        load.wait()

    def states(m, _):
        @pl.when(m == 0)
        def _():
            take = pltpu.make_async_copy(x_ref, x_s, local.at[0])
            take.start()
            take.wait()
            put = pltpu.make_async_copy(x_s, all_ref.at[0], local.at[0])
            put.start()
            put.wait()

        @pl.when(m > 0)
        def _():
            for s in range(bits):
                x_copy(x_piece(m, s), m - 1, 0, s).wait_recv()
            for k in range(1, bits):
                @pl.when(m < (1 << k))
                def _():
                    for s in range(bits):
                        x_copy(x_piece(m, s), m, k, s).start()
            takes = [pltpu.make_async_copy(x_piece(m, s), x_s.at[pl.ds(s * piece, piece), :], local.at[s]) for s in range(bits)]
            for take in takes:
                take.start()
            for take in takes:
                take.wait()

        @pl.when(m == n // 2)
        def _():
            for s in range(bits):
                wo_copy(s).start()
            for k in range(bits - 1):
                for s in range(bits):
                    dy_copy(dy_ref.at[:, pl.ds(s * part, part)], 0, k, s).start()

        where = [_place(me, turn_bits(m, s, n), bits) for s in range(bits)]
        rows_of = lambda s: slice(s * piece, (s + 1) * piece)
        for i, out in enumerate((q_s, k_s, v_s)):
            t = jnp.dot(x_s[...], w_s[i], preferred_element_type=jnp.float32).astype(out.dtype)
            for s in range(bits):
                u = t[rows_of(s), :]
                if i < 2:
                    a, b = u[:, :half].astype(jnp.float32), u[:, half:].astype(jnp.float32)
                    cos, sin = _angles(turns, where[s], rows_of(s))
                    u = jnp.concatenate([a * cos - b * sin, b * cos + a * sin], axis=1).astype(out.dtype)
                out[pl.ds(pl.multiple_of(where[s] * rows + s * piece, piece), piece), :] = u
        return None

    lax.fori_loop(0, n, states, None)
    done = [pltpu.make_async_copy(a, b, local.at[i]) for i, (a, b) in enumerate(((q_s, q_ref), (k_s, k_ref), (v_s, v_ref)))]
    for copy in done:
        copy.start()
    _look(q_s, k_s, v_s, seen_s, lse_ref, top_s, mix_s)
    done += [pltpu.make_async_copy(seen_s, seen_ref, local.at[3 + bits])]
    done[-1].start()

    def spread(m, _):
        for s in range(bits):
            for h in range(2):
                seen_copy(m + h * (n // 2), s, h).start()
        return None

    lax.fori_loop(0, n // 2, spread, None)
    for s in range(bits):
        wo_copy(s).wait()

    def gradients(m, _):
        @pl.when(m == 0)
        def _():
            takes = [pltpu.make_async_copy(dy_ref.at[:, pl.ds(s * part, part)], dy_s.at[s], local.at[3 + s]) for s in range(bits)]
            for take in takes:
                take.start()
            for take in takes:
                take.wait()
            puts = [pltpu.make_async_copy(dy_s.at[s], halves[s].at[0], local.at[3 + s]) for s in range(bits)]
            for put in puts:
                put.start()
            for put in puts:
                put.wait()

        @pl.when(m > 0)
        def _():
            for s in range(bits):
                dy_copy(halves[s].at[m], m - 1, 0, s).wait_recv()
            for k in range(1, bits - 1):
                @pl.when(m < (1 << k))
                def _():
                    for s in range(bits):
                        dy_copy(halves[s].at[m], m, k, s).start()
            takes = [pltpu.make_async_copy(halves[s].at[m], dy_s.at[s], local.at[3 + s]) for s in range(bits)]
            for take in takes:
                take.start()
            for take in takes:
                take.wait()

        for s in range(bits):
            cols = slice(s * part, (s + 1) * part)
            got = dy_s[s]
            at = turn_bits(m, s, n)
            mine_ref[at] = mine_ref[at] + _dot(got, wo_ref[:, cols], 1, 1)
            theirs_s[s, m] = _dot(got, wo_s[:, cols], 1, 1).astype(theirs_s.dtype)
            their_copy(m, s).start()
        return None

    lax.fori_loop(0, n // 2, gradients, None)
    for copy in done:
        copy.wait()

    def sent(m, _):
        for s in range(bits):
            x_copy(x_piece(m, s), m - 1, 0, s).wait_send()

            @pl.when(m < n // 2)
            def _():
                dy_copy(halves[s].at[m % (n // 2)], m % (n // 2) - 1, 0, s).wait_send()
        return None

    lax.fori_loop(1, n, sent, None)

    def add(m, _):
        for s in range(bits):
            their_copy(m, s).wait()
            at = turn_bits(m + n // 2, s, n)
            mine_ref[at] = mine_ref[at] + got_s[s, m].astype(jnp.float32)
            for h in range(2):
                seen_copy(m + h * (n // 2), s, h).wait()
        return None

    lax.fori_loop(0, n // 2, add, None)

    def give(p, _):
        d_ref[pl.ds(pl.multiple_of(_place(me, p, bits) * rows, rows), rows), :] = mine_ref[p].astype(d_ref.dtype)
        return None

    lax.fori_loop(0, n, give, None)


def gather(bits, x, dy, wq, wk, wv, wo, turns):
    rows, width = x.shape
    n, part, head = 1 << bits, width // bits, wo.shape[0]
    low = x.dtype
    half = n // 2
    vmem, anywhere = pl.BlockSpec(memory_space=pltpu.VMEM), pl.BlockSpec(memory_space=pl.ANY)
    heads, unit = jax.ShapeDtypeStruct((n * rows, head), low), jax.ShapeDtypeStruct((half, rows, head), low)
    dma = pltpu.SemaphoreType.DMA
    out = pl.pallas_call(
        functools.partial(_gather, bits),
        in_specs=[anywhere] * 6 + [vmem] * 4,
        out_specs=[*[anywhere] * (1 + 3 * bits), *[anywhere] * 4, vmem, vmem],
        out_shape=[jax.ShapeDtypeStruct((n, rows, width), low), *[jax.ShapeDtypeStruct((half, rows, part), low)] * bits,
                   *[unit] * (2 * bits), heads, heads, heads, heads, jax.ShapeDtypeStruct((1, n * rows), jnp.float32), heads],
        scratch_shapes=[pltpu.VMEM((rows, width), low), pltpu.VMEM((bits, rows, part), low), pltpu.VMEM((3, width, head), low), pltpu.VMEM((head, width), low),
                        pltpu.VMEM((head, width), low), pltpu.VMEM((bits, half, rows, head), low), pltpu.VMEM((bits, half, rows, head), low),
                        pltpu.VMEM((n, rows, head), jnp.float32), *[pltpu.VMEM((n * rows, head), low)] * 4,
                        pltpu.VMEM((1, BLOCK), jnp.float32), pltpu.VMEM((head + 8, BLOCK), jnp.float32), dma((n, bits)), dma((n, bits)), dma((half, bits)), dma((half, bits)),
                        dma((bits,)), dma((bits,)), dma((half, bits)), dma((half, bits)), dma((n, bits)), dma((4 + bits,))],
        compiler_params=pltpu.CompilerParams(collective_id=1, has_side_effects=True, vmem_limit_bytes=VMEM),
        cost_estimate=pl.CostEstimate(flops=2 * n * rows * width * 4 * head, transcendentals=0, bytes_accessed=6 * n * rows * width),
    )(x, dy, wq, wk, wv, wo, *turns)
    return out[0], out[1 : 1 + bits], out[1 + bits : 1 + 2 * bits], out[1 + 2 * bits : 1 + 3 * bits], out[1 + 3 * bits :]


def _sum_all(bits, term_ref, out_ref, got, send, recv):
    n = got.shape[0]
    me = lax.axis_index("tp")
    peers = [_place(me, p, bits) for p in range(n)]
    barrier = pltpu.get_barrier_semaphore()
    for p in range(1, n):
        pl.semaphore_signal(barrier, inc=1, device_id={"tp": peers[p]}, device_id_type=MESH)
    pl.semaphore_wait(barrier, n - 1)

    def copy(p, slot):
        return pltpu.make_async_remote_copy(src_ref=term_ref, dst_ref=got.at[slot], send_sem=send.at[p], recv_sem=recv.at[slot],
                                            device_id={"tp": peers[p]}, device_id_type=MESH)

    for p in range(1, n):
        copy(p, me).start()
    got[me] = term_ref[...]
    for p in range(1, n):
        copy(p, peers[p]).wait_recv()
    total = got[0]
    for i in range(1, n):
        total = total + got[i]
    out_ref[...] = total
    for p in range(1, n):
        copy(p, me).wait_send()


def sum_all(bits, term):
    n = 1 << bits
    vmem, dma = pl.BlockSpec(memory_space=pltpu.VMEM), pltpu.SemaphoreType.DMA
    return pl.pallas_call(
        functools.partial(_sum_all, bits),
        in_specs=[vmem],
        out_specs=vmem,
        out_shape=jax.ShapeDtypeStruct(term.shape, term.dtype),
        scratch_shapes=[pltpu.VMEM((n, *term.shape), term.dtype), dma((n,)), dma((n,))],
        compiler_params=pltpu.CompilerParams(collective_id=2, has_side_effects=True),
        cost_estimate=pl.CostEstimate(flops=10**6, transcendentals=0, bytes_accessed=n * term.size * 4),
    )(term)


def solution(mesh):
    n = mesh.shape["tp"]
    bits = n.bit_length() - 1
    low = bits // 2
    gray = lambda i: i ^ (i >> 1)
    label = [gray(i >> low) | gray(i & ((1 << low) - 1)) << (bits - low) for i in range(n)]
    place = [label.index(v) for v in range(n)]
    pairs = [[(i, place[label[i] ^ (1 << d)]) for i in range(n)] for d in range(bits)]
    nearest = [[label[i] ^ label[j] for j in range(n)] for i in range(n)]

    def hop(t, d):
        return lax.ppermute(t, "tp", pairs[d])

    def pick(t, chosen):
        for d, v in chosen.items():
            axis = bits - 1 - d
            if t.shape[axis] > 1:
                t = lax.slice_in_dim(t, v, v + 1, axis=axis)
        return t

    def flat(t):
        return t.reshape(-1, t.shape[-1])

    def step(x, dy, gain, wq, wk, wv, wo):
        rows, width = x.shape
        part = width // bits
        rel = jnp.array(nearest, jnp.int32)[lax.axis_index("tp")]
        f32 = dict(preferred_element_type=jnp.float32)

        wide = x.astype(jnp.float32)
        scale = lax.rsqrt(jnp.mean(wide * wide, -1, keepdims=True) + 1e-6)
        unit = wide * scale
        wide_gain = gain.astype(jnp.float32)
        tokens = n * rows
        turns = rotations(n, rows, HEAD // 2)
        a, half, moved, given, (q, k, v, seen, lse, d_seen) = gather(bits, (unit * wide_gain).astype(jnp.bfloat16), dy, wq, wk, wv, wo, turns)
        wq, wk, wv, _ = lax.optimization_barrier((wq, wk, wv, a))
        w = jnp.concatenate([wq, wk, wv], 1)
        a = a.reshape(tokens, width)
        across = [(s + bits - 1) % bits for s in range(bits)]

        other = []
        for s in range(bits):
            other.append(hop(given[s], across[s]))
        grads = look_back(rel, q, k, v, d_seen, seen, lse, turns, rows)
        back_dims = (((1,), (1,)), ((), ()))
        cube = lambda t: t.reshape(*(2,) * bits, rows, t.shape[-1])

        w = [lax.slice_in_dim(w, s * part, (s + 1) * part, axis=0) for s in range(bits)]
        got = [[] for _ in range(bits)]
        plain = grads
        grads = cube(grads)

        def term(s, chosen):
            mine = pick(grads, chosen)
            total = lax.dot_general(flat(mine), w[s], back_dims, **f32).reshape(*mine.shape[:-1], part)
            for fixed, r in got[s]:
                if all(chosen[d] == v for d, v in fixed.items()):
                    total = total + pick(r, chosen).astype(jnp.float32)
            return total

        for t in range(bits):
            new = []
            for later in (({(t + 1): 1}, {(t + 1): 0}) if t < SPLIT else ({},)):
                fixed = [{(s + i) % bits: v for i, v in (*((i, int(i == t)) for i in range(t + 1)), *later.items())} for s in range(bits)]
                sent = [term(s, fixed[s]).astype(jnp.bfloat16) for s in range(bits)]
                new += [(s, {**fixed[s], (s + t) % bits: 0}, hop(sent[s], (s + t) % bits)) for s in range(bits)]
            for s, f, r in new:
                got[s].append((f, r))
            if t == 0:
                in_order, *_ = lax.optimization_barrier((flat(plain), *sent))
        by_a = jnp.concatenate([flat(term(s, {d: 0 for d in range(bits)})) for s in range(bits)], 1)

        over = (((0,), (0,)), ((), ()))
        by_w = [lax.dot_general(a, in_order[:, i * HEAD : (i + 1) * HEAD], over, **f32).astype(jnp.bfloat16) for i in range(3)]
        by_wo = [lax.dot_general(flat(other[s]), flat(half[s]), over, **f32).astype(jnp.bfloat16) for s in range(bits)]
        by_wo = [hop(t, across[s]) for s, t in enumerate(by_wo)]
        by_wo = jnp.concatenate([(lax.dot_general(flat(moved[s]), flat(half[s]), over, **f32) + by_wo[s].astype(jnp.float32)).astype(jnp.bfloat16)
                                 for s in range(bits)], 1)

        by_gain = jnp.sum(by_a * unit, 0, keepdims=True)
        by_gain = sum_all(bits, by_gain)
        g = by_a * wide_gain
        by_x = scale * (g - unit * jnp.mean(g * unit, -1, keepdims=True)) + dy.astype(jnp.float32)
        return (by_x.astype(jnp.bfloat16), by_gain, *by_w, by_wo)

    tokens, columns = P(("dp", "tp"), None), P(None, "tp")
    return jax.shard_map(
        step,
        mesh=mesh,
        in_specs=(tokens, tokens, P(None), columns, columns, columns, P("tp", None)),
        out_specs=(tokens, P("dp", None), P("dp", "tp"), P("dp", "tp"), P("dp", "tp"), P(("dp", "tp"), None)),
        check_vma=False,
    )
```

```python
import functools

import jax
import jax.numpy as jnp
from jax import lax
from jax.experimental import pallas as pl
from jax.experimental.pallas import tpu as pltpu
from jax.sharding import PartitionSpec as P

NEG = -1e30
HIDDEN = 2 * NEG
LOG2E = 1.4426950408889634
VMEM = 62 * 2**20
STRIP = 512
BLOCK = 1024


HEAD = 256
THETA = 10000
SPLIT = 2
WEIGH = {"0b": (0, 1), "1a": (2, 3)}


def rotations(blocks, rows, half):
    speed = THETA ** (-jnp.arange(half, dtype=jnp.float32) / half)
    first, inside = (jnp.arange(blocks) * rows).astype(jnp.float32)[:, None, None] * speed, jnp.arange(rows).astype(jnp.float32)[:, None] * speed
    return jnp.cos(first), jnp.sin(first), jnp.cos(inside), jnp.sin(inside)


def _angles(turns, block, rows=slice(None)):
    first_cos, first_sin, cos, sin = turns
    c, s, ci, si = first_cos[block], first_sin[block], cos[rows, :], sin[rows, :]
    return c * ci - s * si, s * ci + c * si


def _dot(a, b, ca, cb):
    return lax.dot_general(a, b, (((ca,), (cb,)), ((), ())), preferred_element_type=jnp.float32)


def _visible():
    shape = (STRIP, STRIP)
    return lax.broadcasted_iota(jnp.int32, shape, 1) >= lax.broadcasted_iota(jnp.int32, shape, 0)


def _rows(ref, first, count):
    return ref.at[pl.ds(pl.multiple_of(first, STRIP), count), :]


def _over_keys(iq, block):
    lax.fori_loop(0, iq, lambda j, _: block(j * BLOCK, BLOCK, range(BLOCK // STRIP), None), None)
    for strip in range(BLOCK // STRIP):
        block(iq * BLOCK + strip * STRIP, STRIP, range(strip, BLOCK // STRIP), strip)


def _look(q_ref, k_ref, v_ref, out_ref, lse_ref, top_s, mix_s):
    tokens, head = q_ref.shape
    scale = head**-0.5
    e = scale * LOG2E

    def queries(iq, _):
        top_s[...] = jnp.full(top_s.shape, NEG, jnp.float32)
        mix_s[...] = jnp.zeros(mix_s.shape, jnp.float32)

        def block(first, keys, strips, masked):
            k = _rows(k_ref, first, keys)[...]
            scores = [_dot(k, _rows(q_ref, iq * BLOCK + n * STRIP, STRIP)[...], 1, 1) for n in strips]
            values = jnp.concatenate([_rows(v_ref, first, keys)[...].T, jnp.ones((8, keys), k.dtype)], axis=0)
            weights, keeps = [], []
            for n, s in zip(strips, scores):
                at = slice(n * STRIP, (n + 1) * STRIP)
                if n == masked:
                    s = jnp.where(_visible(), s, HIDDEN)
                old = top_s[:, at]
                top = jnp.maximum(old, s.max(axis=0, keepdims=True))
                top_s[:, at] = top
                weights.append(jnp.exp2((s - top) * e).astype(k.dtype))
                keeps.append(jnp.exp2((old - top) * e))
            for n, p, keep in zip(strips, weights, keeps):
                at = slice(n * STRIP, (n + 1) * STRIP)
                mix_s[:, at] = mix_s[:, at] * keep + _dot(values, p, 1, 0)

        _over_keys(iq, block)
        total = mix_s[head : head + 1, :]
        _rows(out_ref, iq * BLOCK, BLOCK)[...] = (mix_s[:head, :] * (1 / total)).T.astype(out_ref.dtype)
        lse_ref[:, pl.ds(pl.multiple_of(iq * BLOCK, BLOCK), BLOCK)] = top_s[...] * scale + jnp.log(total)

    lax.fori_loop(0, tokens // BLOCK, queries, None)


def _look_back(bits, q_ref, k_ref, v_ref, do_ref, seen_ref, lse_ref, *refs):
    turns, (out_ref, dq_s, dk_s, dv_s) = refs[:4], refs[4:]
    head, low = q_ref.shape[1], q_ref.dtype
    rows, half = out_ref.shape[1], head // 2
    scale = head**-0.5
    e = scale * LOG2E
    iq, me = pl.program_id(0), lax.axis_index("tp")

    def finish(block, at, value):
        cos, sin = _angles(turns, block)
        a, b = value[:, :half], value[:, half:]
        place = _way(me, block, bits)
        out_ref[place, :, at : at + half] = (a * cos + b * sin).astype(low)
        out_ref[place, :, at + half : at + head] = (b * cos - a * sin).astype(low)

    @pl.when(iq == 0)
    def _():
        dk_s[...] = jnp.zeros_like(dk_s)
        dv_s[...] = jnp.zeros_like(dv_s)

    dq_s[...] = jnp.zeros_like(dq_s)
    lse = lse_ref[...] * LOG2E
    delta = (do_ref[...].astype(jnp.float32) * seen_ref[...].astype(jnp.float32)).T.sum(axis=0, keepdims=True)

    def block(first, keys, strips, masked):
        k, v = _rows(k_ref, first, keys)[...], _rows(v_ref, first, keys)[...]
        ats = [slice(n * STRIP, (n + 1) * STRIP) for n in strips]
        qs, dos = [q_ref[at, :] for at in ats], [do_ref[at, :] for at in ats]
        scores = [_dot(k, x, 1, 1) for x in qs]
        dps = [_dot(v, x, 1, 1) for x in dos]
        for n, at, q, do, s, dp in zip(strips, ats, qs, dos, scores, dps):
            p = jnp.exp2(s * e - lse[:, at])
            if n == masked:
                p = jnp.where(_visible(), p, 0.0)
            ds = (p * (dp - delta[:, at])).astype(low)
            dv_at, dk_at = _rows(dv_s, first, keys), _rows(dk_s, first, keys)
            dv_at[...] += _dot(p.astype(low), do, 1, 0)
            dk_at[...] += _dot(ds, q, 1, 0)
            dq_s[:, at] += _dot(k.T, ds, 1, 0)

    _over_keys(iq, block)
    dq = (dq_s[...] * scale).T.astype(low).astype(jnp.float32)
    each = BLOCK // rows
    for i in range(each):
        finish(iq * each + i, 0, dq[i * rows : (i + 1) * rows, :])

    @pl.when(iq == pl.num_programs(0) - 1)
    def _():
        def keys(i, _):
            at = pl.ds(pl.multiple_of(i * rows, rows), rows)
            finish(i, head, (dk_s[at, :] * scale).astype(low).astype(jnp.float32))
            out_ref[_way(me, i, bits), :, 2 * head :] = dv_s[at, :].astype(low)

        lax.fori_loop(0, out_ref.shape[0], keys, None)


def look_back(bits, q, k, v, do, seen, lse, turns, rows):
    tokens, head = q.shape
    once = dict(pipeline_mode=pl.Buffered(1))
    whole = lambda shape: pl.BlockSpec(shape, lambda i: (0,) * len(shape), **once)
    block = pl.BlockSpec((BLOCK, head), lambda i: (i, 0))
    out = (tokens // rows, rows, 3 * head)
    return pl.pallas_call(
        functools.partial(_look_back, bits),
        grid_spec=pl.GridSpec(
            grid=(tokens // BLOCK,),
            in_specs=[block, whole(k.shape), whole(v.shape), block, block, pl.BlockSpec((1, BLOCK), lambda i: (0, i)), *[whole(t.shape) for t in turns]],
            out_specs=whole(out),
            scratch_shapes=[pltpu.VMEM((head, BLOCK), jnp.float32), pltpu.VMEM((tokens, head), jnp.float32), pltpu.VMEM((tokens, head), jnp.float32)],
        ),
        out_shape=jax.ShapeDtypeStruct(out, q.dtype),
        compiler_params=pltpu.CompilerParams(dimension_semantics=("arbitrary",), vmem_limit_bytes=VMEM),
        cost_estimate=pl.CostEstimate(flops=5 * tokens * tokens * head, transcendentals=tokens * tokens, bytes_accessed=16 * q.size),
    )(q, k, v, do, seen, lse, *turns)


def _way(me, other, bits):
    low = bits // 2
    side = 1 << low
    way = 0
    for one, two, first in ((me // side, other // side, 0), (me % side, other % side, low)):
        for b in range(low):
            way = way + (one // (1 << b) + one // (1 << (b + 1)) + two // (1 << b) + two // (1 << (b + 1))) % 2 * (1 << (first + b))
    return way


MESH = pl.DeviceIdType.MESH


def turn_bits(m, s, n):
    return (m * (1 << s)) % n + (m * (1 << s)) // n


def _place(me, flip, bits):
    low = bits // 2
    side = 1 << low
    found = 0
    for at, first in ((me // side, 0), (me % side, low)):
        above, out = 0, 0
        for b in reversed(range(low)):
            bit = (at // (1 << b) + (at // (1 << (b + 1)) if b + 1 < low else 0)) % 2
            bit = (bit + flip // (1 << (first + b))) % 2
            above = (above + bit) % 2
            out = out + above * (1 << b)
        found = found * side + out
    return found


def _gather(bits, x_ref, dy_ref, wq_ref, wk_ref, wv_ref, wo_in, *refs):
    turns, refs = refs[:4], refs[4:]
    all_ref, halves, moved = refs[0], refs[1 : 1 + bits], refs[1 + bits : 1 + 3 * bits]
    q_ref, k_ref, v_ref, seen_ref, w_ref, lse_ref, d_ref = refs[1 + 3 * bits : 8 + 3 * bits]
    x_s, dy_s, w_s, wo_ref, wo_s, theirs_s, got_s, mine_ref, q_s, k_s, v_s, seen_s, top_s, mix_s = refs[8 + 3 * bits : 22 + 3 * bits]
    x_send, x_recv, dy_send, dy_recv, wo_send, wo_recv, their_send, their_recv, out_sem, local = refs[22 + 3 * bits :]
    n, rows, width = all_ref.shape
    head = q_ref.shape[1]
    half = head // 2
    piece, part = rows // bits, width // bits
    me = lax.axis_index("tp")
    peers = [{"tp": _place(me, 1 << d, bits)} for d in range(bits)]

    barrier = pltpu.get_barrier_semaphore()
    for peer in peers:
        pl.semaphore_signal(barrier, inc=1, device_id=peer, device_id_type=MESH)
    pl.semaphore_wait(barrier, bits)

    def x_piece(m, s):
        return all_ref.at[turn_bits(m, s, n), pl.ds(s * piece, piece), :]

    def x_copy(src, m, k, s):
        return pltpu.make_async_remote_copy(src_ref=src, dst_ref=x_piece(m + (1 << k), s), send_sem=x_send.at[m + (1 << k), s],
                                            recv_sem=x_recv.at[m + (1 << k), s], device_id=peers[(s + k) % bits], device_id_type=MESH)

    def dy_copy(src, m, k, s):
        return pltpu.make_async_remote_copy(src_ref=src, dst_ref=halves[s].at[m + (1 << k)], send_sem=dy_send.at[m + (1 << k), s],
                                            recv_sem=dy_recv.at[m + (1 << k), s], device_id=peers[(s + k) % bits], device_id_type=MESH)

    def wo_copy(s):
        here = (slice(None), pl.ds(s * part, part))
        return pltpu.make_async_remote_copy(src_ref=wo_in.at[here], dst_ref=wo_s.at[here], send_sem=wo_send.at[s], recv_sem=wo_recv.at[s],
                                            device_id=peers[(s + bits - 1) % bits], device_id_type=MESH)

    def their_copy(m, s):
        return pltpu.make_async_remote_copy(src_ref=theirs_s.at[s, m], dst_ref=got_s.at[s, m], send_sem=their_send.at[m, s],
                                            recv_sem=their_recv.at[m, s], device_id=peers[(s + bits - 1) % bits], device_id_type=MESH)

    def seen_copy(m, s, h):
        block = _place(me, turn_bits(m, s, n), bits)
        return pltpu.make_async_copy(seen_s.at[pl.ds(pl.multiple_of(block * rows, rows), rows), :], moved[h * bits + s].at[m % (n // 2)], out_sem.at[m, s])

    for k in range(bits):
        for s in range(bits):
            x_copy(x_ref.at[pl.ds(s * piece, piece), :], 0, k, s).start()
    loads = [pltpu.make_async_copy(a, b, local.at[3 + i]) for i, (a, b) in enumerate([(wq_ref, w_s.at[0]), (wk_ref, w_s.at[1]), (wv_ref, w_s.at[2]), (wo_in, wo_ref)])]
    for load in loads:
        load.start()
    mine_ref[...] = jnp.zeros_like(mine_ref)
    for load in loads:
        load.wait()

    def states(m, _):
        @pl.when(m == 0)
        def _():
            take = pltpu.make_async_copy(x_ref, x_s, local.at[0])
            take.start()
            take.wait()
            put = pltpu.make_async_copy(x_s, all_ref.at[0], local.at[0])
            put.start()
            put.wait()

        @pl.when(m > 0)
        def _():
            for s in range(bits):
                x_copy(x_piece(m, s), m - 1, 0, s).wait_recv()
            for k in range(1, bits):
                @pl.when(m < (1 << k))
                def _():
                    for s in range(bits):
                        x_copy(x_piece(m, s), m, k, s).start()
            takes = [pltpu.make_async_copy(x_piece(m, s), x_s.at[pl.ds(s * piece, piece), :], local.at[s]) for s in range(bits)]
            for take in takes:
                take.start()
            for take in takes:
                take.wait()

        @pl.when(m == n // 2)
        def _():
            for s in range(bits):
                wo_copy(s).start()
            for k in range(bits - 1):
                for s in range(bits):
                    dy_copy(dy_ref.at[:, pl.ds(s * part, part)], 0, k, s).start()

        where = [_place(me, turn_bits(m, s, n), bits) for s in range(bits)]
        rows_of = lambda s: slice(s * piece, (s + 1) * piece)
        for i, out in enumerate((q_s, k_s, v_s)):
            t = jnp.dot(x_s[...], w_s[i], preferred_element_type=jnp.float32).astype(out.dtype)
            for s in range(bits):
                u = t[rows_of(s), :]
                if i < 2:
                    a, b = u[:, :half].astype(jnp.float32), u[:, half:].astype(jnp.float32)
                    cos, sin = _angles(turns, where[s], rows_of(s))
                    u = jnp.concatenate([a * cos - b * sin, b * cos + a * sin], axis=1).astype(out.dtype)
                out[pl.ds(pl.multiple_of(where[s] * rows + s * piece, piece), piece), :] = u
        return None

    lax.fori_loop(0, n, states, None)
    done = [pltpu.make_async_copy(a, b, local.at[i]) for i, (a, b) in enumerate(((q_s, q_ref), (k_s, k_ref), (v_s, v_ref)))]
    for copy in done:
        copy.start()
    _look(q_s, k_s, v_s, seen_s, lse_ref, top_s, mix_s)
    for i, (a, b) in enumerate([(seen_s, seen_ref), *((w_s.at[i], w_ref.at[:, pl.ds(i * head, head)]) for i in range(3))]):
        done += [pltpu.make_async_copy(a, b, local.at[3 + bits + i])]
        done[-1].start()

    def spread(m, _):
        for s in range(bits):
            for h in range(2):
                seen_copy(m + h * (n // 2), s, h).start()
        return None

    lax.fori_loop(0, n // 2, spread, None)
    for s in range(bits):
        wo_copy(s).wait()

    def gradients(m, _):
        @pl.when(m == 0)
        def _():
            takes = [pltpu.make_async_copy(dy_ref.at[:, pl.ds(s * part, part)], dy_s.at[s], local.at[3 + s]) for s in range(bits)]
            for take in takes:
                take.start()
            for take in takes:
                take.wait()
            puts = [pltpu.make_async_copy(dy_s.at[s], halves[s].at[0], local.at[3 + s]) for s in range(bits)]
            for put in puts:
                put.start()
            for put in puts:
                put.wait()

        @pl.when(m > 0)
        def _():
            for s in range(bits):
                dy_copy(halves[s].at[m], m - 1, 0, s).wait_recv()
            for k in range(1, bits - 1):
                @pl.when(m < (1 << k))
                def _():
                    for s in range(bits):
                        dy_copy(halves[s].at[m], m, k, s).start()
            takes = [pltpu.make_async_copy(halves[s].at[m], dy_s.at[s], local.at[3 + s]) for s in range(bits)]
            for take in takes:
                take.start()
            for take in takes:
                take.wait()

        for s in range(bits):
            cols = slice(s * part, (s + 1) * part)
            got = dy_s[s]
            at = turn_bits(m, s, n)
            mine_ref[at] = mine_ref[at] + _dot(got, wo_ref[:, cols], 1, 1)
            theirs_s[s, m] = _dot(got, wo_s[:, cols], 1, 1).astype(theirs_s.dtype)
            their_copy(m, s).start()
        return None

    lax.fori_loop(0, n // 2, gradients, None)
    for copy in done:
        copy.wait()

    def sent(m, _):
        for s in range(bits):
            x_copy(x_piece(m, s), m - 1, 0, s).wait_send()

            @pl.when(m < n // 2)
            def _():
                dy_copy(halves[s].at[m % (n // 2)], m % (n // 2) - 1, 0, s).wait_send()
        return None

    lax.fori_loop(1, n, sent, None)

    def add(m, _):
        for s in range(bits):
            their_copy(m, s).wait()
            at = turn_bits(m + n // 2, s, n)
            mine_ref[at] = mine_ref[at] + got_s[s, m].astype(jnp.float32)
            for h in range(2):
                seen_copy(m + h * (n // 2), s, h).wait()
        return None

    lax.fori_loop(0, n // 2, add, None)

    def give(p, _):
        d_ref[pl.ds(pl.multiple_of(_place(me, p, bits) * rows, rows), rows), :] = mine_ref[p].astype(d_ref.dtype)
        return None

    lax.fori_loop(0, n, give, None)


def gather(bits, x, dy, wq, wk, wv, wo, turns):
    rows, width = x.shape
    n, part, head = 1 << bits, width // bits, wo.shape[0]
    low = x.dtype
    half = n // 2
    vmem, anywhere = pl.BlockSpec(memory_space=pltpu.VMEM), pl.BlockSpec(memory_space=pl.ANY)
    heads, unit = jax.ShapeDtypeStruct((n * rows, head), low), jax.ShapeDtypeStruct((half, rows, head), low)
    dma = pltpu.SemaphoreType.DMA
    out = pl.pallas_call(
        functools.partial(_gather, bits),
        in_specs=[anywhere] * 6 + [vmem] * 4,
        out_specs=[*[anywhere] * (1 + 3 * bits), *[anywhere] * 5, vmem, vmem],
        out_shape=[jax.ShapeDtypeStruct((n, rows, width), low), *[jax.ShapeDtypeStruct((half, rows, part), low)] * bits,
                   *[unit] * (2 * bits), heads, heads, heads, heads, jax.ShapeDtypeStruct((width, 3 * head), low), jax.ShapeDtypeStruct((1, n * rows), jnp.float32), heads],
        scratch_shapes=[pltpu.VMEM((rows, width), low), pltpu.VMEM((bits, rows, part), low), pltpu.VMEM((3, width, head), low), pltpu.VMEM((head, width), low),
                        pltpu.VMEM((head, width), low), pltpu.VMEM((bits, half, rows, head), low), pltpu.VMEM((bits, half, rows, head), low),
                        pltpu.VMEM((n, rows, head), jnp.float32), *[pltpu.VMEM((n * rows, head), low)] * 4,
                        pltpu.VMEM((1, BLOCK), jnp.float32), pltpu.VMEM((head + 8, BLOCK), jnp.float32), dma((n, bits)), dma((n, bits)), dma((half, bits)), dma((half, bits)),
                        dma((bits,)), dma((bits,)), dma((half, bits)), dma((half, bits)), dma((n, bits)), dma((7 + bits,))],
        compiler_params=pltpu.CompilerParams(collective_id=1, has_side_effects=True, vmem_limit_bytes=VMEM),
        cost_estimate=pl.CostEstimate(flops=2 * n * rows * width * 4 * head, transcendentals=0, bytes_accessed=6 * n * rows * width),
    )(x, dy, wq, wk, wv, wo, *turns)
    return out[0], out[1 : 1 + bits], out[1 + bits : 1 + 2 * bits], out[1 + 2 * bits : 1 + 3 * bits], out[1 + 3 * bits :]


def _sum_all(bits, term_ref, out_ref, got, send, recv):
    n = got.shape[0]
    me = lax.axis_index("tp")
    peers = [_place(me, p, bits) for p in range(n)]
    barrier = pltpu.get_barrier_semaphore()
    for p in range(1, n):
        pl.semaphore_signal(barrier, inc=1, device_id={"tp": peers[p]}, device_id_type=MESH)
    pl.semaphore_wait(barrier, n - 1)

    def copy(p, slot):
        return pltpu.make_async_remote_copy(src_ref=term_ref, dst_ref=got.at[slot], send_sem=send.at[p], recv_sem=recv.at[slot],
                                            device_id={"tp": peers[p]}, device_id_type=MESH)

    for p in range(1, n):
        copy(p, me).start()
    got[me] = term_ref[...]
    for p in range(1, n):
        copy(p, peers[p]).wait_recv()
    total = got[0]
    for i in range(1, n):
        total = total + got[i]
    out_ref[...] = total
    for p in range(1, n):
        copy(p, me).wait_send()


def sum_all(bits, term):
    n = 1 << bits
    vmem, dma = pl.BlockSpec(memory_space=pltpu.VMEM), pltpu.SemaphoreType.DMA
    return pl.pallas_call(
        functools.partial(_sum_all, bits),
        in_specs=[vmem],
        out_specs=vmem,
        out_shape=jax.ShapeDtypeStruct(term.shape, term.dtype),
        scratch_shapes=[pltpu.VMEM((n, *term.shape), term.dtype), dma((n,)), dma((n,))],
        compiler_params=pltpu.CompilerParams(collective_id=2, has_side_effects=True),
        cost_estimate=pl.CostEstimate(flops=10**6, transcendentals=0, bytes_accessed=n * term.size * 4),
    )(term)


def solution(mesh):
    n = mesh.shape["tp"]
    bits = n.bit_length() - 1
    low = bits // 2
    gray = lambda i: i ^ (i >> 1)
    label = [gray(i >> low) | gray(i & ((1 << low) - 1)) << (bits - low) for i in range(n)]
    place = [label.index(v) for v in range(n)]
    pairs = [[(i, place[label[i] ^ (1 << d)]) for i in range(n)] for d in range(bits)]

    def hop(t, d):
        return lax.ppermute(t, "tp", pairs[d])

    def pick(t, chosen):
        for d, v in chosen.items():
            axis = bits - 1 - d
            if t.shape[axis] > 1:
                t = lax.slice_in_dim(t, v, v + 1, axis=axis)
        return t

    def flat(t):
        return t.reshape(-1, t.shape[-1])

    def step(x, dy, gain, wq, wk, wv, wo):
        rows, width = x.shape
        part = width // bits
        f32 = dict(preferred_element_type=jnp.float32)

        wide = x.astype(jnp.float32)
        scale = lax.rsqrt(jnp.mean(wide * wide, -1, keepdims=True) + 1e-6)
        unit = wide * scale
        wide_gain = gain.astype(jnp.float32)
        tokens = n * rows
        turns = rotations(n, rows, HEAD // 2)
        a, half, moved, given, (q, k, v, seen, w, lse, d_seen) = gather(bits, (unit * wide_gain).astype(jnp.bfloat16), dy, wq, wk, wv, wo, turns)
        a = a.reshape(tokens, width)
        across = [(s + bits - 1) % bits for s in range(bits)]

        other = []
        for s in range(bits):
            other.append(hop(given[s], across[s]))
        grads = look_back(bits, q, k, v, d_seen, seen, lse, turns, rows)
        back_dims = (((1,), (1,)), ((), ()))
        cube = lambda t: t.reshape(*(2,) * bits, rows, t.shape[-1])

        w = [lax.slice_in_dim(w, s * part, (s + 1) * part, axis=0) for s in range(bits)]
        got = [[] for _ in range(bits)]
        plain = grads
        grads = cube(grads)

        def term(s, chosen):
            mine = pick(grads, chosen)
            total = lax.dot_general(flat(mine), w[s], back_dims, **f32).reshape(*mine.shape[:-1], part)
            for fixed, r in got[s]:
                if all(chosen[d] == v for d, v in fixed.items()):
                    total = total + pick(r, chosen).astype(jnp.float32)
            return total

        over = (((0,), (0,)), ((), ()))
        by_w, by_wo = [None] * bits, [None] * bits

        def after(t, sent):
            return lax.optimization_barrier((t, *sent))[0]

        base = plain
        for t in range(bits):
            new = []
            for later in (({(t + 1): 1}, {(t + 1): 0}) if t < SPLIT else ({},)):
                first = later.get(t + 1, 0) == 1
                stage = f"{t}{'a' if first else 'b'}"
                fixed = [{(s + i) % bits: v for i, v in (*((i, int(i == t)) for i in range(t + 1)), *later.items())} for s in range(bits)]
                sent = []
                for s in range(bits):
                    sent.append(term(s, fixed[s]).astype(jnp.bfloat16))
                for s in range(bits):
                    new += [(s, {**fixed[s], (s + t) % bits: 0}, hop(sent[s], (s + t) % bits))]
                if t == 0:
                    base = after(base, sent)
                    grads = cube(base)
                for s in WEIGH.get(stage, ()):
                    over_rows = lax.slice_in_dim(a, s * part, (s + 1) * part, axis=1)
                    by_w[s] = lax.dot_general(over_rows, flat(after(base, sent)), over, **f32).astype(jnp.bfloat16)
                for s in range(bits) if stage == "1a" else ():
                    by_wo[s] = lax.dot_general(flat(after(other[s], sent)), flat(half[s]), over, **f32).astype(jnp.bfloat16)
                    by_wo[s] = hop(by_wo[s], across[s])
                for s in range(bits) if stage == "1b" else ():
                    mine = lax.dot_general(flat(after(moved[s], sent)), flat(half[s]), over, **f32)
                    by_wo[s] = (mine + by_wo[s].astype(jnp.float32)).astype(jnp.bfloat16)
            for s, f, r in new:
                got[s].append((f, r))
        by_a = jnp.concatenate([flat(term(s, {d: 0 for d in range(bits)})) for s in range(bits)], 1)
        by_w = [jnp.concatenate([t[:, i * HEAD : (i + 1) * HEAD] for t in by_w], 0) for i in range(3)]
        by_wo = jnp.concatenate(by_wo, 1)

        by_gain = jnp.sum(by_a * unit, 0, keepdims=True)
        by_gain = sum_all(bits, by_gain)
        g = by_a * wide_gain
        by_x = scale * (g - unit * jnp.mean(g * unit, -1, keepdims=True)) + dy.astype(jnp.float32)
        return (by_x.astype(jnp.bfloat16), by_gain, *by_w, by_wo)

    tokens, columns = P(("dp", "tp"), None), P(None, "tp")
    return jax.shard_map(
        step,
        mesh=mesh,
        in_specs=(tokens, tokens, P(None), columns, columns, columns, P("tp", None)),
        out_specs=(tokens, P("dp", None), P("dp", "tp"), P("dp", "tp"), P("dp", "tp"), P(("dp", "tp"), None)),
        check_vma=False,
    )
```
